32 devices in a mesh: groups: 2 (over y), depth: 4 (over z), dirfreq: 2 (over x), shot: 2 (over core).
Axes of the slice: x: 2, y: 2, z: 4, core: 2. Of those that a mesh axis runs over, the one named last changes fastest.
Arguments:
- codes: bfloat16 [4, 2, 2, 1024, 1024], P('depth', 'dirfreq', None, 'shot'), may hold values from -128 to 127, as said below
- row_scale: float32 [4, 2, 1024], P('depth', 'dirfreq'), may hold values from 0 to 1, as said below
- refl_index: int32 [8, 1024], P(('groups', 'depth')), parts along dimension 0, may hold values from 0 to 127
- refl_table: float32 [128], replicated, may hold values from -0.3 to 0.3
- fields_in: bfloat16 [8, 2, 2, 96, 1024], P(('groups', 'depth'), 'dirfreq', None, 'shot'), parts along dimension 0, may hold values from -6 to 6
Outputs:
- wavefields: bfloat16 [8, 2, 2, 96, 1024], P(('groups', 'depth'), 'dirfreq', None, 'shot'), parts along dimension 0
The draws below stay inside these ranges and needn't reach their ends.
There are 2 independent parts, one for each index of `groups`. The reference program is written for one: setup_inputs(seed, part) draws one part's arguments, and reference() takes and returns one part's arrays. A program takes and returns all parts, laid end to end along the dimension named above; an argument that names none is the same for every part. Nothing has to cross between parts.
Inputs may be any that keep to these rules, and one draw needn't show every extreme that they name: `codes`: whole numbers. `row_scale`: positive.
All inputs are finite; a program needn't handle non-finite values.
Results may differ from the reference program's by a relative error of at most 0.03.
Values may be sent and summed in bfloat16 or wider, within the bound.
A program may use at most 64 MiB of HBM per device.

```python
import math
import jax
import jax.numpy as jnp
from jax import lax

X = 1024
CLASSES = 128
SHOTS = 96
LEVELS = 4
FREQ = 1


def draw_codes(key, part):
    values = jax.random.randint(key, (LEVELS, 2 * FREQ, 2, X, X), -128, 128, dtype=jnp.int32)
    return values.astype(jnp.float32).astype(jnp.bfloat16)


def draw_row_scale(key, part):
    shape = (LEVELS, 2 * FREQ, X)
    spread = jax.random.uniform(key, shape, jnp.float32, math.log(0.5), math.log(2.0))
    return jnp.exp(spread) / (121.0 * math.sqrt(X))


def place_ends(result, key, smallest, high):
    dims = result.shape
    place = [jax.random.randint(jax.random.fold_in(key, axis), (), 0, dims[axis]) for axis in range(len(dims))]
    result = result.at[tuple(place)].set(smallest)
    longest = dims.index(max(dims))
    place[longest] = (place[longest] + 1) % dims[longest]
    return result.at[tuple(place)].set(high)


def steps_of(rng, dims, cuts, least, high):
    gain = 1.0
    for axis_at, parts in cuts:
        draws = jax.random.uniform(jax.random.fold_in(jax.random.fold_in(rng, 6), axis_at), (parts,), jnp.float32, least / len(cuts), high / len(cuts))
        gain = gain * jnp.repeat(jnp.exp(draws), dims[axis_at] // parts).reshape((-1,) + (1,) * (len(dims) - 1 - axis_at))
    return gain


def gaussian(stream_key, dims, scale, limit, cuts=(), kind=jnp.bfloat16):
    factor_of = steps_of(stream_key, dims, cuts, -0.22, 0.18) if cuts else 1.0
    entries = jax.random.normal(stream_key, dims, jnp.float32) * scale * factor_of
    return jnp.minimum(jnp.maximum(entries, -limit), limit).astype(kind)


def setup_inputs(seed: int = 0, part: int = 0) -> dict:
    keys = jax.random.split(jax.random.key(seed), 6)
    own_keys = jax.random.split(jax.random.fold_in(keys[5], part), 6)
    return {
        "codes": draw_codes(jax.random.fold_in(keys[5], 71), part),
        "row_scale": draw_row_scale(jax.random.fold_in(keys[5], 71), part),
        "refl_index": place_ends(jax.random.randint(own_keys[2], (LEVELS, X), 0, CLASSES), jax.random.fold_in(own_keys[2], 1), 0, CLASSES - 1).astype(jnp.int32),
        "refl_table": jnp.clip(jax.random.uniform(keys[3], (CLASSES,), jnp.float32, -0.3, 0.3), -0.3, 0.3),
        "fields_in": gaussian(own_keys[4], (LEVELS, 2 * FREQ, 2, SHOTS, X), 1.0, 6.0, ((0, 4), (1, 2), (3, 2))),
    }


def contract(left, right):
    return lax.dot_general(left, right, (((1,), (1,)), ((), ())), preferred_element_type=jnp.float32)


def extrapolate(operator_full, scales, field):
    real_part = contract(field[0], operator_full[0]) - contract(field[1], operator_full[1])
    imag_part = contract(field[0], operator_full[1]) + contract(field[1], operator_full[0])
    return (jnp.stack([real_part, imag_part]) * scales[None, None, :]).astype(jnp.bfloat16)


def reference(codes, row_scale, refl_index, refl_table, fields_in):
    classes = refl_table.shape[0]
    onehot = (refl_index[:, :, None] == jnp.arange(classes, dtype=jnp.int32)[None, None, :]).astype(jnp.float32)
    reflect_all = jnp.einsum("lxk,k->lx", onehot, refl_table, precision=lax.Precision.HIGHEST)
    half = codes.shape[1] // 2
    start = jnp.zeros(fields_in.shape[2:], jnp.bfloat16)
    downs = []
    ups = []
    for freq in range(half):
        def down_step(carry, inputs):
            operator_full, scales, reflect, source, previous = inputs
            arrived = (-reflect * previous.astype(jnp.float32)).astype(jnp.bfloat16)
            mixed = ((1.0 + reflect) * carry.astype(jnp.float32) + (arrived.astype(jnp.float32) + source.astype(jnp.float32))).astype(jnp.bfloat16)
            produced = extrapolate(operator_full, scales, mixed)
            sending = (reflect * carry.astype(jnp.float32)).astype(jnp.bfloat16)
            return produced, (produced, sending)

        final_down, (downgoing, sent) = lax.scan(down_step, start, (codes[:, freq], row_scale[:, freq], reflect_all, fields_in[:, freq], fields_in[:, half + freq]))

        def up_step(carry, inputs):
            operator_full, scales, reflect, arrived = inputs
            mixed = ((1.0 - reflect) * carry.astype(jnp.float32) + arrived.astype(jnp.float32)).astype(jnp.bfloat16)
            produced = extrapolate(operator_full, scales, mixed)
            return produced, produced

        final_up, upgoing = lax.scan(up_step, start, (codes[:, half + freq], row_scale[:, half + freq], reflect_all, sent), reverse=True)
        downs.append(downgoing)
        ups.append(upgoing)
    return jnp.stack(downs + ups, axis=1)
```

```python
import functools

import jax
import jax.numpy as jnp
from jax import lax
from jax.experimental import pallas as pl
from jax.experimental.pallas import tpu as pltpu
from jax.sharding import PartitionSpec as P

MESH = pl.DeviceIdType.MESH
BLOCK = 256


def kernel(levels, halves, chunks, rows, codes_hbm, scale_hbm, index_hbm, table_hbm, fields_hbm, out_ref,
           own, weights, fields, source, reflect, scale, index, table, chain, side, partner, result,
           load_sem, code_sem, code_send, code_recv, chain_send, chain_recv, side_send, side_recv, part_send):
    depth = lax.axis_index("depth")
    slot = lax.axis_index("dirfreq")
    core = lax.axis_index("shot")
    is_down = slot < halves
    is_up = jnp.logical_not(is_down)
    first, last = depth == 0, depth == levels - 1
    across = jnp.where(is_down, slot + halves, slot - halves)
    ahead = jnp.where(is_down, depth + 1, depth - 1)
    behind = jnp.where(is_down, depth - 1, depth + 1)
    has_next = jnp.where(is_down, jnp.logical_not(last), jnp.logical_not(first))
    has_prev = jnp.where(is_down, jnp.logical_not(first), jnp.logical_not(last))
    has_side = jnp.logical_or(is_down, jnp.logical_not(first))
    down_next = jnp.logical_and(is_down, jnp.logical_not(last))
    up_prev = jnp.logical_and(is_up, jnp.logical_not(first))
    blocks = own.shape[1] // BLOCK
    half = 2 * rows

    small = [pltpu.make_async_copy(a, b, load_sem.at[i]) for i, (a, b) in enumerate(
        ((index_hbm, index), (table_hbm, table), (scale_hbm, scale), (fields_hbm, fields)))]
    for copy in small:
        copy.start()

    def code_load(q, p):
        span = pl.ds(q * BLOCK, BLOCK)
        return pltpu.make_async_copy(codes_hbm.at[0, 0, p, span], own.at[p, span], code_sem.at[q, p])

    pieces = [(q, p) for q in range(blocks) for p in range(2)]
    for q, p in pieces:
        code_load(q, p).start()

    barrier = pltpu.get_barrier_semaphore()

    def greet(device):
        pl.semaphore_signal(barrier, inc=1, device_id=device, device_id_type=MESH)

    greet({"shot": 1 - core})
    greet({"dirfreq": across})

    @pl.when(has_next)
    def _():
        greet({"depth": ahead})

    @pl.when(has_prev)
    def _():
        greet({"depth": behind})

    @pl.when(down_next)
    def _():
        greet({"depth": depth + 1, "dirfreq": across})

    @pl.when(up_prev)
    def _():
        greet({"depth": depth - 1, "dirfreq": across})

    for copy in small[:2]:
        copy.wait()
    classes = table.shape[0]
    row = lax.broadcasted_iota(jnp.int32, (classes, classes), 0)
    column = lax.broadcasted_iota(jnp.int32, (classes, classes), 1)
    entries = jnp.broadcast_to(table[...].reshape(1, classes), (classes, classes))
    upright = jnp.sum(jnp.where(row == column, entries, 0.0), axis=1, keepdims=True)
    width = index.shape[1]
    picked = lax.broadcasted_iota(jnp.int32, (classes, width), 0) == index[...]
    reflect[...] = jnp.sum(jnp.where(picked, upright, 0.0), axis=0, keepdims=True)

    for copy in small[2:]:
        copy.wait()
    per = 16 // rows
    for m in range(chunks // per):
        for p in range(2):
            values = fields[0, 0, p, m * 16:(m + 1) * 16].astype(jnp.float32)
            for t in range(per):
                source[m * per + t, p * rows:(p + 1) * rows] = values[t * rows:(t + 1) * rows]

    wanted = (2 + has_next.astype(jnp.int32) + has_prev.astype(jnp.int32)
              + jnp.logical_or(down_next, up_prev).astype(jnp.int32))
    pl.semaphore_wait(barrier, wanted)

    def part_copy(k):
        return pltpu.make_async_remote_copy(
            src_ref=partner.at[k], dst_ref=side.at[k], send_sem=part_send.at[k], recv_sem=side_recv.at[k],
            device_id={"dirfreq": across}, device_id_type=MESH)

    @pl.when(is_up)
    def _():
        for k in range(chunks):
            partner[k] = (-reflect[...] * source[k]).astype(jnp.bfloat16)
            part_copy(k).start()

    @pl.when(jnp.logical_not(has_prev))
    def _():
        chain[...] = jnp.zeros_like(chain)

    @pl.when(jnp.logical_not(has_side))
    def _():
        side[...] = jnp.zeros_like(side)

    def code_copy(q, p):
        here = weights.at[core, q, p]
        return pltpu.make_async_remote_copy(
            src_ref=here, dst_ref=here, send_sem=code_send.at[q, p], recv_sem=code_recv.at[q, p],
            device_id={"shot": 1 - core}, device_id_type=MESH)

    def code_arrival(q, p):
        there = weights.at[1 - core, q, p]
        return pltpu.make_async_remote_copy(
            src_ref=there, dst_ref=there, send_sem=code_send.at[q, p], recv_sem=code_recv.at[q, p],
            device_id={"shot": 1 - core}, device_id_type=MESH)

    for q, p in pieces:
        code_load(q, p).wait()
        weights[core, q, p] = own[p, q * BLOCK:(q + 1) * BLOCK].T
        code_copy(q, p).start()

    def chain_copy(k):
        return pltpu.make_async_remote_copy(
            src_ref=result.at[k], dst_ref=chain.at[k], send_sem=chain_send.at[k], recv_sem=chain_recv.at[k],
            device_id={"depth": ahead}, device_id_type=MESH)

    def side_copy(k):
        return pltpu.make_async_remote_copy(
            src_ref=result.at[k], dst_ref=side.at[k], send_sem=side_send.at[k], recv_sem=side_recv.at[k],
            device_id={"depth": depth + 1, "dirfreq": across}, device_id_type=MESH)

    sign = jnp.where(is_down, 1.0, -1.0).astype(jnp.float32)

    def step(k, opening):
        @pl.when(has_side)
        def _():
            part_copy(k).wait_recv()

        @pl.when(has_prev)
        def _():
            chain_copy(k).wait_recv()

        beside = side[k].astype(jnp.float32)
        base = jnp.where(is_down, beside + source[k],
                         (reflect[...] * beside).astype(jnp.bfloat16).astype(jnp.float32))
        mixed = ((1.0 + sign * reflect[...]) * chain[k].astype(jnp.float32) + base).astype(jnp.bfloat16)
        for t in range(2):
            holder = core if t == 0 else 1 - core
            for q in range(blocks):
                if opening and t == 1:
                    code_arrival(q, 0).wait_recv()
                    code_arrival(q, 1).wait_recv()
                by_real = jnp.dot(mixed, weights[holder, q, 0], preferred_element_type=jnp.float32)
                by_imag = jnp.dot(mixed, weights[holder, q, 1], preferred_element_type=jnp.float32)
                real = by_real[:rows] - by_imag[rows:]
                imag = by_imag[:rows] + by_real[rows:]
                columns = pl.ds(pl.multiple_of((holder * blocks + q) * BLOCK, BLOCK), BLOCK)
                both = jnp.concatenate([real, imag], axis=0) * scale[0, :, columns]
                result[k, :, columns] = both.astype(jnp.bfloat16)

        @pl.when(has_next)
        def _():
            chain_copy(k).start()

        @pl.when(down_next)
        def _():
            side_copy(k).start()

    step(0, True)

    @pl.loop(1, chunks)
    def _(k):
        step(k, False)

    for m in range(chunks // per):
        for p in range(2):
            parts = [result[m * per + t].astype(jnp.float32)[p * rows:(p + 1) * rows] for t in range(per)]
            out_ref[0, 0, p, m * 16:(m + 1) * 16] = jnp.concatenate(parts, axis=0).astype(jnp.bfloat16)

    for q, p in pieces:
        code_copy(q, p).wait_send()

    @pl.when(is_up)
    def _():
        for k in range(chunks):
            part_copy(k).wait_send()

    @pl.when(has_next)
    def _():
        for k in range(chunks):
            chain_copy(k).wait_send()

    @pl.when(down_next)
    def _():
        for k in range(chunks):
            side_copy(k).wait_send()


def shards(codes, row_scale, refl_index, refl_table, fields_in):
    levels = lax.axis_size("depth")
    halves = lax.axis_size("dirfreq") // 2
    shots, width = fields_in.shape[3:]
    rows = 8
    chunks = shots // rows
    held = codes.shape[3]
    blocks = held // BLOCK
    dma = pltpu.SemaphoreType.DMA
    wave = (chunks, 2 * rows, width)
    any_space = pl.BlockSpec(memory_space=pltpu.HBM)
    return pl.pallas_call(
        functools.partial(kernel, levels, halves, chunks, rows),
        out_shape=jax.ShapeDtypeStruct(fields_in.shape, jnp.bfloat16),
        in_specs=[any_space] * 5,
        out_specs=pl.BlockSpec(memory_space=pltpu.VMEM),
        scratch_shapes=[
            pltpu.VMEM((2, held, width), jnp.bfloat16),
            pltpu.VMEM((2, blocks, 2, width, BLOCK), jnp.bfloat16),
            pltpu.VMEM(fields_in.shape, jnp.bfloat16),
            pltpu.VMEM(wave, jnp.float32),
            pltpu.VMEM((1, width), jnp.float32),
            pltpu.VMEM(row_scale.shape, jnp.float32),
            pltpu.VMEM(refl_index.shape, jnp.int32),
            pltpu.VMEM(refl_table.shape, jnp.float32),
            pltpu.VMEM(wave, jnp.bfloat16),
            pltpu.VMEM(wave, jnp.bfloat16),
            pltpu.VMEM(wave, jnp.bfloat16),
            pltpu.VMEM(wave, jnp.bfloat16),
            dma((4,)),
            dma((blocks, 2)),
            dma((blocks, 2)),
            dma((blocks, 2)),
            dma((chunks,)),
            dma((chunks,)),
            dma((chunks,)),
            dma((chunks,)),
            dma((chunks,)),
        ],
        compiler_params=pltpu.CompilerParams(collective_id=0, has_side_effects=True, vmem_limit_bytes=40 * 2**20),
    )(codes, row_scale, refl_index, refl_table, fields_in)


def solution(mesh):
    placed = (
        P("depth", "dirfreq", None, "shot", None),
        P("depth", "dirfreq", None),
        P(("groups", "depth"), None),
        P(),
        P(("groups", "depth"), "dirfreq", None, "shot", None),
    )
    return jax.shard_map(
        shards,
        mesh=mesh,
        in_specs=placed,
        out_specs=P(("groups", "depth"), "dirfreq", None, "shot", None),
        check_vma=False,
    )
```

```python
import functools

import jax
import jax.numpy as jnp
from jax import lax
from jax.experimental import pallas as pl
from jax.experimental.pallas import tpu as pltpu
from jax.sharding import PartitionSpec as P

MESH = pl.DeviceIdType.MESH
BLOCK = 256


def kernel(levels, halves, chunks, rows, codes_hbm, scale_hbm, index_hbm, table_hbm, fields_hbm, out_ref,
           own, weights, fields, source, reflect, scale, index, table, chain, side, partner, result,
           load_sem, code_sem, code_send, code_recv, chain_send, chain_recv, side_send, side_recv, part_send):
    depth = lax.axis_index("depth")
    slot = lax.axis_index("dirfreq")
    core = lax.axis_index("shot")
    is_down = slot < halves
    is_up = jnp.logical_not(is_down)
    first, last = depth == 0, depth == levels - 1
    across = jnp.where(is_down, slot + halves, slot - halves)
    ahead = jnp.where(is_down, depth + 1, depth - 1)
    behind = jnp.where(is_down, depth - 1, depth + 1)
    has_next = jnp.where(is_down, jnp.logical_not(last), jnp.logical_not(first))
    has_prev = jnp.where(is_down, jnp.logical_not(first), jnp.logical_not(last))
    has_side = jnp.logical_or(is_down, jnp.logical_not(first))
    down_next = jnp.logical_and(is_down, jnp.logical_not(last))
    up_prev = jnp.logical_and(is_up, jnp.logical_not(first))
    blocks = own.shape[1] // BLOCK
    half = 2 * rows

    small = [pltpu.make_async_copy(a, b, load_sem.at[i]) for i, (a, b) in enumerate(
        ((index_hbm, index), (table_hbm, table), (scale_hbm, scale), (fields_hbm, fields)))]
    for copy in small:
        copy.start()

    def code_load(q, p):
        span = pl.ds(q * BLOCK, BLOCK)
        return pltpu.make_async_copy(codes_hbm.at[0, 0, p, span], own.at[p, span], code_sem.at[q, p])

    pieces = [(q, p) for q in range(blocks) for p in range(2)]
    for q, p in pieces:
        code_load(q, p).start()

    barrier = pltpu.get_barrier_semaphore()

    def greet(device):
        pl.semaphore_signal(barrier, inc=1, device_id=device, device_id_type=MESH)

    greet({"shot": 1 - core})
    greet({"dirfreq": across})

    @pl.when(has_next)
    def _():
        greet({"depth": ahead})

    @pl.when(has_prev)
    def _():
        greet({"depth": behind})

    @pl.when(down_next)
    def _():
        greet({"depth": depth + 1, "dirfreq": across})

    @pl.when(up_prev)
    def _():
        greet({"depth": depth - 1, "dirfreq": across})

    for copy in small[:2]:
        copy.wait()
    classes = table.shape[0]
    row = lax.broadcasted_iota(jnp.int32, (classes, classes), 0)
    column = lax.broadcasted_iota(jnp.int32, (classes, classes), 1)
    entries = jnp.broadcast_to(table[...].reshape(1, classes), (classes, classes))
    upright = jnp.sum(jnp.where(row == column, entries, 0.0), axis=1, keepdims=True)
    width = index.shape[1]
    picked = lax.broadcasted_iota(jnp.int32, (classes, width), 0) == index[...]
    reflect[...] = jnp.sum(jnp.where(picked, upright, 0.0), axis=0, keepdims=True)

    for copy in small[2:]:
        copy.wait()
    per = 16 // rows
    for m in range(chunks // per):
        for p in range(2):
            values = fields[0, 0, p, m * 16:(m + 1) * 16].astype(jnp.float32)
            for t in range(per):
                source[m * per + t, p * rows:(p + 1) * rows] = values[t * rows:(t + 1) * rows]

    wanted = (2 + has_next.astype(jnp.int32) + has_prev.astype(jnp.int32)
              + jnp.logical_or(down_next, up_prev).astype(jnp.int32))
    pl.semaphore_wait(barrier, wanted)

    def part_copy(k):
        return pltpu.make_async_remote_copy(
            src_ref=partner.at[k], dst_ref=side.at[k], send_sem=part_send.at[k], recv_sem=side_recv.at[k],
            device_id={"dirfreq": across}, device_id_type=MESH)

    @pl.when(is_up)
    def _():
        for k in range(chunks):
            partner[k] = (-reflect[...] * source[k]).astype(jnp.bfloat16)
            part_copy(k).start()

    @pl.when(jnp.logical_not(has_prev))
    def _():
        chain[...] = jnp.zeros_like(chain)

    @pl.when(jnp.logical_not(has_side))
    def _():
        side[...] = jnp.zeros_like(side)

    def code_copy(q, p):
        here = weights.at[core, q, p]
        return pltpu.make_async_remote_copy(
            src_ref=here, dst_ref=here, send_sem=code_send.at[q, p], recv_sem=code_recv.at[q, p],
            device_id={"shot": 1 - core}, device_id_type=MESH)

    def code_arrival(q, p):
        there = weights.at[1 - core, q, p]
        return pltpu.make_async_remote_copy(
            src_ref=there, dst_ref=there, send_sem=code_send.at[q, p], recv_sem=code_recv.at[q, p],
            device_id={"shot": 1 - core}, device_id_type=MESH)

    for q, p in pieces:
        code_load(q, p).wait()
        weights[core, q, p] = own[p, q * BLOCK:(q + 1) * BLOCK].T
        code_copy(q, p).start()

    def chain_copy(k):
        return pltpu.make_async_remote_copy(
            src_ref=result.at[k], dst_ref=chain.at[k], send_sem=chain_send.at[k], recv_sem=chain_recv.at[k],
            device_id={"depth": ahead}, device_id_type=MESH)

    def side_copy(k):
        return pltpu.make_async_remote_copy(
            src_ref=result.at[k], dst_ref=side.at[k], send_sem=side_send.at[k], recv_sem=side_recv.at[k],
            device_id={"depth": depth + 1, "dirfreq": across}, device_id_type=MESH)

    sign = jnp.where(is_down, 1.0, -1.0).astype(jnp.float32)

    def step(k, opening):
        @pl.when(has_side)
        def _():
            part_copy(k).wait_recv()

        @pl.when(has_prev)
        def _():
            chain_copy(k).wait_recv()

        beside = side[k].astype(jnp.float32)
        base = jnp.where(is_down, beside + source[k],
                         (reflect[...] * beside).astype(jnp.bfloat16).astype(jnp.float32))
        mixed = ((1.0 + sign * reflect[...]) * chain[k].astype(jnp.float32) + base).astype(jnp.bfloat16)
        for t in range(2):
            holder = core if t == 0 else 1 - core
            for q in range(blocks):
                if opening and t == 1:
                    code_arrival(q, 0).wait_recv()
                    code_arrival(q, 1).wait_recv()
                by_real = jnp.dot(mixed, weights[holder, q, 0], preferred_element_type=jnp.float32)
                by_imag = jnp.dot(mixed, weights[holder, q, 1], preferred_element_type=jnp.float32)
                real = by_real[:rows] - by_imag[rows:]
                imag = by_imag[:rows] + by_real[rows:]
                columns = pl.ds(pl.multiple_of((holder * blocks + q) * BLOCK, BLOCK), BLOCK)
                both = jnp.concatenate([real, imag], axis=0) * scale[0, :, columns]
                result[k, :, columns] = both.astype(jnp.bfloat16)

        @pl.when(has_next)
        def _():
            chain_copy(k).start()

        @pl.when(down_next)
        def _():
            side_copy(k).start()

    step(0, True)

    @pl.loop(1, chunks)
    def _(k):
        step(k, False)

    for m in range(chunks // per):
        for p in range(2):
            parts = [result[m * per + t].astype(jnp.float32)[p * rows:(p + 1) * rows] for t in range(per)]
            out_ref[0, 0, p, m * 16:(m + 1) * 16] = jnp.concatenate(parts, axis=0).astype(jnp.bfloat16)

    for q, p in pieces:
        code_copy(q, p).wait_send()

    @pl.when(is_up)
    def _():
        for k in range(chunks):
            part_copy(k).wait_send()

    @pl.when(has_next)
    def _():
        for k in range(chunks):
            chain_copy(k).wait_send()

    @pl.when(down_next)
    def _():
        for k in range(chunks):
            side_copy(k).wait_send()


def shards(codes, row_scale, refl_index, refl_table, fields_in):
    levels = lax.axis_size("depth")
    halves = lax.axis_size("dirfreq") // 2
    shots, width = fields_in.shape[3:]
    rows = 8
    chunks = shots // rows
    held = codes.shape[3]
    blocks = held // BLOCK
    dma = pltpu.SemaphoreType.DMA
    wave = (chunks, 2 * rows, width)
    any_space = pl.BlockSpec(memory_space=pltpu.HBM)
    return pl.pallas_call(
        functools.partial(kernel, levels, halves, chunks, rows),
        out_shape=jax.ShapeDtypeStruct(fields_in.shape, jnp.bfloat16),
        in_specs=[any_space] * 5,
        out_specs=pl.BlockSpec(memory_space=pltpu.VMEM),
        scratch_shapes=[
            pltpu.VMEM((2, held, width), jnp.bfloat16),
            pltpu.VMEM((2, blocks, 2, width, BLOCK), jnp.bfloat16),
            pltpu.VMEM(fields_in.shape, jnp.bfloat16),
            pltpu.VMEM(wave, jnp.float32),
            pltpu.VMEM((1, width), jnp.float32),
            pltpu.VMEM(row_scale.shape, jnp.float32),
            pltpu.VMEM(refl_index.shape, jnp.int32),
            pltpu.VMEM(refl_table.shape, jnp.float32),
            pltpu.VMEM(wave, jnp.bfloat16),
            pltpu.VMEM(wave, jnp.bfloat16),
            pltpu.VMEM(wave, jnp.bfloat16),
            pltpu.VMEM(wave, jnp.bfloat16),
            dma((4,)),
            dma((blocks, 2)),
            dma((blocks, 2)),
            dma((blocks, 2)),
            dma((chunks,)),
            dma((chunks,)),
            dma((chunks,)),
            dma((chunks,)),
            dma((chunks,)),
        ],
        compiler_params=pltpu.CompilerParams(collective_id=0, has_side_effects=True, vmem_limit_bytes=67043328),
    )(codes, row_scale, refl_index, refl_table, fields_in)


def solution(mesh):
    placed = (
        P("depth", "dirfreq", None, "shot", None),
        P("depth", "dirfreq", None),
        P(("groups", "depth"), None),
        P(),
        P(("groups", "depth"), "dirfreq", None, "shot", None),
    )
    return jax.shard_map(
        shards,
        mesh=mesh,
        in_specs=placed,
        out_specs=P(("groups", "depth"), "dirfreq", None, "shot", None),
        check_vma=False,
    )
```

```python
import functools

import jax
import jax.numpy as jnp
from jax import lax
from jax.experimental import pallas as pl
from jax.experimental.pallas import tpu as pltpu
from jax.sharding import PartitionSpec as P

MESH = pl.DeviceIdType.MESH
BLOCK = 256


def kernel(levels, halves, chunks, rows, codes_hbm, scale_hbm, index_hbm, table_hbm, fields_hbm, out_ref,
           own, weights, fields, source, reflect, scale, index, table, chain, side, partner, result,
           load_sem, code_sem, code_send, code_recv, chain_send, chain_recv, side_send, side_recv, part_send, ready):
    depth = lax.axis_index("depth")
    slot = lax.axis_index("dirfreq")
    core = lax.axis_index("shot")
    is_down = slot < halves
    is_up = jnp.logical_not(is_down)
    first, last = depth == 0, depth == levels - 1
    across = jnp.where(is_down, slot + halves, slot - halves)
    ahead = jnp.where(is_down, depth + 1, depth - 1)
    behind = jnp.where(is_down, depth - 1, depth + 1)
    has_next = jnp.where(is_down, jnp.logical_not(last), jnp.logical_not(first))
    has_prev = jnp.where(is_down, jnp.logical_not(first), jnp.logical_not(last))
    has_side = jnp.logical_or(is_down, jnp.logical_not(first))
    down_next = jnp.logical_and(is_down, jnp.logical_not(last))
    blocks = own.shape[1] // BLOCK
    part_width = own.shape[1]

    small = [pltpu.make_async_copy(a, b, load_sem.at[i]) for i, (a, b) in enumerate(
        ((index_hbm, index), (table_hbm, table), (scale_hbm, scale), (fields_hbm, fields)))]
    for copy in small:
        copy.start()

    def code_load(q, p):
        span = pl.ds(q * BLOCK, BLOCK)
        return pltpu.make_async_copy(codes_hbm.at[0, 0, p, span], own.at[p, span], code_sem.at[q, p])

    pieces = [(q, p) for q in range(blocks) for p in range(2)]
    for q, p in pieces:
        code_load(q, p).start()

    barrier = pltpu.get_barrier_semaphore()

    def greet(device):
        pl.semaphore_signal(barrier, inc=1, device_id=device, device_id_type=MESH)

    greet({"shot": 1 - core})
    greet({"dirfreq": across})

    @pl.when(has_next)
    def _():
        greet({"depth": ahead})

    @pl.when(has_prev)
    def _():
        greet({"depth": behind})

    for copy in small[:2]:
        copy.wait()
    classes = table.shape[0]
    row = lax.broadcasted_iota(jnp.int32, (classes, classes), 0)
    column = lax.broadcasted_iota(jnp.int32, (classes, classes), 1)
    entries = jnp.broadcast_to(table[...].reshape(1, classes), (classes, classes))
    upright = jnp.sum(jnp.where(row == column, entries, 0.0), axis=1, keepdims=True)
    width = index.shape[1]
    picked = lax.broadcasted_iota(jnp.int32, (classes, width), 0) == index[...]
    reflect[...] = jnp.sum(jnp.where(picked, upright, 0.0), axis=0, keepdims=True)

    for copy in small[2:]:
        copy.wait()
    per = 16 // rows
    for m in range(chunks // per):
        for p in range(2):
            values = fields[0, 0, p, m * 16:(m + 1) * 16].astype(jnp.float32)
            for t in range(per):
                source[m * per + t, p * rows:(p + 1) * rows] = values[t * rows:(t + 1) * rows]

    pl.semaphore_wait(barrier, 2 + has_next.astype(jnp.int32) + has_prev.astype(jnp.int32))

    @pl.when(jnp.logical_and(is_down, has_prev))
    def _():
        pl.semaphore_signal(ready, inc=1, device_id={"depth": behind}, device_id_type=MESH)

    def span_of(h):
        return pl.ds(pl.multiple_of(h * part_width, BLOCK), part_width)

    def part_copy(k, h):
        return pltpu.make_async_remote_copy(
            src_ref=partner.at[k, h], dst_ref=side.at[k, h], send_sem=part_send.at[k, h], recv_sem=side_recv.at[k, h],
            device_id={"dirfreq": across}, device_id_type=MESH)

    both = [(0, core), (1, 1 - core)]

    @pl.when(is_up)
    def _():
        for k in range(chunks):
            for _, h in both:
                span = span_of(h)
                partner[k, h] = (-reflect[:, span] * source[k, :, span]).astype(jnp.bfloat16)
                part_copy(k, h).start()

    @pl.when(jnp.logical_not(has_prev))
    def _():
        chain[...] = jnp.zeros_like(chain)

    @pl.when(jnp.logical_not(has_side))
    def _():
        side[...] = jnp.zeros_like(side)

    def code_copy(q, p):
        here = weights.at[core, q, p]
        return pltpu.make_async_remote_copy(
            src_ref=here, dst_ref=here, send_sem=code_send.at[q, p], recv_sem=code_recv.at[q, p],
            device_id={"shot": 1 - core}, device_id_type=MESH)

    def code_arrival(q, p):
        there = weights.at[1 - core, q, p]
        return pltpu.make_async_remote_copy(
            src_ref=there, dst_ref=there, send_sem=code_send.at[q, p], recv_sem=code_recv.at[q, p],
            device_id={"shot": 1 - core}, device_id_type=MESH)

    for q, p in pieces:
        code_load(q, p).wait()
        weights[core, q, p] = own[p, q * BLOCK:(q + 1) * BLOCK].T
        code_copy(q, p).start()

    def chain_copy(k, h):
        return pltpu.make_async_remote_copy(
            src_ref=result.at[k, h], dst_ref=chain.at[k, h], send_sem=chain_send.at[k, h], recv_sem=chain_recv.at[k, h],
            device_id={"depth": ahead}, device_id_type=MESH)

    def side_copy(k, h):
        return pltpu.make_async_remote_copy(
            src_ref=result.at[k, h], dst_ref=side.at[k, h], send_sem=side_send.at[k, h], recv_sem=side_recv.at[k, h],
            device_id={"depth": depth + 1, "dirfreq": across}, device_id_type=MESH)

    sign = jnp.where(is_down, 1.0, -1.0).astype(jnp.float32)

    def mixed_half(k, h):
        @pl.when(has_side)
        def _():
            part_copy(k, h).wait_recv()

        @pl.when(has_prev)
        def _():
            chain_copy(k, h).wait_recv()

        span = span_of(h)
        ratio = reflect[:, span]
        beside = side[k, h].astype(jnp.float32)
        base = jnp.where(is_down, beside + source[k, :, span],
                         (ratio * beside).astype(jnp.bfloat16).astype(jnp.float32))
        return ((1.0 + sign * ratio) * chain[k, h].astype(jnp.float32) + base).astype(jnp.bfloat16)

    def step(k, opening):
        sums = {}
        early, late = both[0][1], both[1][1]
        mixed = mixed_half(k, early)
        for t, holder in both:
            for q in range(blocks):
                if opening and t == 1:
                    code_arrival(q, 0).wait_recv()
                    code_arrival(q, 1).wait_recv()
                for p in range(2):
                    sums[t, q, p] = jnp.dot(mixed, weights[holder, q, p, span_of(early)],
                                            preferred_element_type=jnp.float32)
        mixed = mixed_half(k, late)
        if opening:
            @pl.when(down_next)
            def _():
                pl.semaphore_wait(ready, 1)

        for t, holder in both:
            for q in range(blocks):
                by_real, by_imag = (
                    sums[t, q, p] + jnp.dot(mixed, weights[holder, q, p, span_of(late)],
                                            preferred_element_type=jnp.float32) for p in range(2))
                real = by_real[:rows] - by_imag[rows:]
                imag = by_imag[:rows] + by_real[rows:]
                columns = pl.ds(pl.multiple_of((holder * blocks + q) * BLOCK, BLOCK), BLOCK)
                pair = jnp.concatenate([real, imag], axis=0) * scale[0, :, columns]
                result[k, holder, :, q * BLOCK:(q + 1) * BLOCK] = pair.astype(jnp.bfloat16)

            @pl.when(has_next)
            def _():
                chain_copy(k, holder).start()

            @pl.when(down_next)
            def _():
                side_copy(k, holder).start()

    step(0, True)

    @pl.loop(1, chunks)
    def _(k):
        step(k, False)

    for m in range(chunks // per):
        for h in range(2):
            for p in range(2):
                parts = [result[m * per + t, h].astype(jnp.float32)[p * rows:(p + 1) * rows] for t in range(per)]
                out_ref[0, 0, p, m * 16:(m + 1) * 16, h * part_width:(h + 1) * part_width] = (
                    jnp.concatenate(parts, axis=0).astype(jnp.bfloat16))

    for q, p in pieces:
        code_copy(q, p).wait_send()

    def drain(flag, copy):
        @pl.when(flag)
        def _():
            for k in range(chunks):
                for h in range(2):
                    copy(k, h).wait_send()

    drain(is_up, part_copy)
    drain(has_next, chain_copy)
    drain(down_next, side_copy)


def shards(codes, row_scale, refl_index, refl_table, fields_in):
    levels = lax.axis_size("depth")
    halves = lax.axis_size("dirfreq") // 2
    shots, width = fields_in.shape[3:]
    rows = 8
    chunks = shots // rows
    held = codes.shape[3]
    blocks = held // BLOCK
    dma = pltpu.SemaphoreType.DMA
    wave = (chunks, 2 * rows, width)
    halved = (chunks, 2, 2 * rows, held)
    any_space = pl.BlockSpec(memory_space=pltpu.HBM)
    return pl.pallas_call(
        functools.partial(kernel, levels, halves, chunks, rows),
        out_shape=jax.ShapeDtypeStruct(fields_in.shape, jnp.bfloat16),
        in_specs=[any_space] * 5,
        out_specs=pl.BlockSpec(memory_space=pltpu.VMEM),
        scratch_shapes=[
            pltpu.VMEM((2, held, width), jnp.bfloat16),
            pltpu.VMEM((2, blocks, 2, width, BLOCK), jnp.bfloat16),
            pltpu.VMEM(fields_in.shape, jnp.bfloat16),
            pltpu.VMEM(wave, jnp.float32),
            pltpu.VMEM((1, width), jnp.float32),
            pltpu.VMEM(row_scale.shape, jnp.float32),
            pltpu.VMEM(refl_index.shape, jnp.int32),
            pltpu.VMEM(refl_table.shape, jnp.float32),
            pltpu.VMEM(halved, jnp.bfloat16),
            pltpu.VMEM(halved, jnp.bfloat16),
            pltpu.VMEM(halved, jnp.bfloat16),
            pltpu.VMEM(halved, jnp.bfloat16),
            dma((4,)),
            dma((blocks, 2)),
            dma((blocks, 2)),
            dma((blocks, 2)),
            dma((chunks, 2)),
            dma((chunks, 2)),
            dma((chunks, 2)),
            dma((chunks, 2)),
            dma((chunks, 2)),
            pltpu.SemaphoreType.REGULAR,
        ],
        compiler_params=pltpu.CompilerParams(collective_id=0, has_side_effects=True, vmem_limit_bytes=67043328),
    )(codes, row_scale, refl_index, refl_table, fields_in)


def solution(mesh):
    placed = (
        P("depth", "dirfreq", None, "shot", None),
        P("depth", "dirfreq", None),
        P(("groups", "depth"), None),
        P(),
        P(("groups", "depth"), "dirfreq", None, "shot", None),
    )
    return jax.shard_map(
        shards,
        mesh=mesh,
        in_specs=placed,
        out_specs=P(("groups", "depth"), "dirfreq", None, "shot", None),
        check_vma=False,
    )
```
